32 devices in a mesh: lon: 4 (over x, core), lat: 8 (over z, y).
Axes of the slice: x: 2, y: 2, z: 4, core: 2. Of those that a mesh axis runs over, the one named last changes fastest.
Arguments:
- u_vel: float32 [16, 128, 4320], P(None, 'lat', 'lon'), may hold values from -6 to 6
- v_vel: float32 [16, 128, 4320], P(None, 'lat', 'lon'), may hold values from -6 to 6
- u_mask: int32 [16, 128, 4320], P(None, 'lat', 'lon'), may hold values 0 or 1
- v_mask: int32 [16, 128, 4320], P(None, 'lat', 'lon'), may hold values 0 or 1
- t_mask: int32 [16, 128, 4320], P(None, 'lat', 'lon'), may hold values 0 or 1
- bottom: int32 [128, 4320], P('lat', 'lon'), may hold values from 0 to 16
- inv_dx: float32 [128, 4320], P('lat', 'lon'), may hold values from 0.5 to 2
- inv_dy: float32 [128, 4320], P('lat', 'lon'), may hold values from 0.5 to 2
Outputs:
- flux_spectrum: float32 [16, 128, 2160], P(None, ('lat', 'lon'))
The draws below stay inside these ranges and needn't reach their ends.
All inputs are finite; a program needn't handle non-finite values. No bound on the sum of `u_mask` or of `v_mask` or of `t_mask` on one device may be relied on, other than what follows from the above.
Results may differ from the reference program's by a relative error of at most 0.0003.
Values sent between devices are 32-bit elements; how exact they have to be, the bound alone decides.
A program may use at most 64 MiB of HBM per device.

```python
import math
import jax
import jax.numpy as jnp
from jax import lax

NI = 4320
K = 16
NJ = 128
NM = 2160


def touch_ends(array, rng, low, high):
    index_at = [jax.random.randint(jax.random.fold_in(rng, axis), (), 0, length) for axis, length in enumerate(array.shape)]
    widest = array.shape.index(max(array.shape))
    next_to = index_at[:widest] + [(index_at[widest] + 1) % array.shape[widest]] + index_at[widest + 1:]
    return array.at[tuple(index_at)].set(low).at[tuple(next_to)].set(high)


def level_of(stream_key, shape, split, low, top_value):
    def one(axis_at, blocks):
        steps = jax.random.uniform(jax.random.fold_in(jax.random.fold_in(stream_key, 6), axis_at), (blocks,), jnp.float32, low / len(split), top_value / len(split))
        return jnp.repeat(jnp.exp(steps), shape[axis_at] // blocks).reshape((-1,) + (1,) * (len(shape) - axis_at - 1))

    loudness = one(*split[0])
    for cut in split[1:]:
        loudness = loudness * one(*cut)
    return loudness


def normal_values(stream_key, dims, scale, bound, split=(), kind=jnp.bfloat16):
    values = scale * jax.random.normal(stream_key, dims, jnp.float32)
    if split:
        values = values * level_of(stream_key, dims, split, -0.22, 0.18)
    return jnp.clip(values, -bound, bound).astype(kind)


def setup_inputs(seed: int = 0) -> dict:
    key_of = jax.random.split(jax.random.key(seed), 9)
    u_vel = normal_values(key_of[0], (K, NJ, NI), 1.0, 6.0, ((1, 8), (2, 4)), jnp.float32)
    v_vel = normal_values(key_of[1], (K, NJ, NI), 1.0, 6.0, ((1, 8), (2, 4)), jnp.float32)
    u_mask = touch_ends((jax.random.randint(key_of[2], (K, NJ, NI), 0, 4) < 3).astype(jnp.int32), jax.random.fold_in(key_of[2], 1), 0, 1)
    v_mask = touch_ends((jax.random.randint(key_of[3], (K, NJ, NI), 0, 4) < 3).astype(jnp.int32), jax.random.fold_in(key_of[3], 1), 0, 1)
    t_mask = touch_ends((jax.random.randint(key_of[4], (K, NJ, NI), 0, 4) < 3).astype(jnp.int32), jax.random.fold_in(key_of[4], 1), 0, 1)
    bottom = touch_ends(jax.random.randint(key_of[5], (NJ, NI), 0, K + 1), jax.random.fold_in(key_of[5], 1), 0, K).astype(jnp.int32)
    inv_dx = jnp.clip(jnp.exp(math.log(2.0) - 1.3862944 * jax.random.uniform(key_of[6], (NJ, NI), jnp.float32) ** level_of(key_of[6], (NJ, NI), ((0, 8), (1, 4)), -0.2, 0.2)), 0.5, 2.0)
    inv_dy = jnp.clip(jnp.exp(math.log(2.0) - 1.3862944 * jax.random.uniform(key_of[7], (NJ, NI), jnp.float32) ** level_of(key_of[7], (NJ, NI), ((0, 8), (1, 4)), -0.2, 0.2)), 0.5, 2.0)
    return {"u_vel": u_vel, "v_vel": v_vel, "u_mask": u_mask, "v_mask": v_mask, "t_mask": t_mask, "bottom": bottom, "inv_dx": inv_dx, "inv_dy": inv_dy}


def level_flux(depth_level_fields, bottom, inv_dx, inv_dy):
    zonal_velocity_slice, meridional_velocity_slice, zonal_mask_slice, meridional_mask_slice, tracer_mask_slice, depth_level_index = depth_level_fields
    live_mask = (depth_level_index < bottom).astype(jnp.float32)
    weight = tracer_mask_slice.astype(jnp.float32) * live_mask
    u_masked = zonal_velocity_slice * zonal_mask_slice.astype(jnp.float32)
    meridional_velocity_masked = meridional_velocity_slice * meridional_mask_slice.astype(jnp.float32)

    def extend(field):
        north_row = -field[-1:, ::-1]
        south_row = jnp.zeros_like(field[:1])
        return jnp.concatenate([south_row, field, north_row], axis=0)

    def along_i(field):
        return (jnp.roll(field, -1, axis=1) - jnp.roll(field, 1, axis=1)) * 0.5 * inv_dx

    def along_j(field):
        extended = extend(field)
        return (extended[2:] - extended[:-2]) * 0.5 * inv_dy

    adv_u = weight * (u_masked * along_i(u_masked) + meridional_velocity_masked * along_j(u_masked))
    adv_v = weight * (u_masked * along_i(meridional_velocity_masked) + meridional_velocity_masked * along_j(meridional_velocity_masked))
    spectra = jnp.fft.rfft(jnp.stack([u_masked, meridional_velocity_masked, adv_u, adv_v]), axis=-1)[..., :NM]
    real_part = jnp.real(spectra)
    imag_part = jnp.imag(spectra)
    cross_terms = (real_part[0] * real_part[2] + imag_part[0] * imag_part[2]
                   + real_part[1] * real_part[3] + imag_part[1] * imag_part[3])
    weights_m = jnp.where(jnp.arange(NM) == 0, 1.0, 2.0).astype(jnp.float32)
    return -weights_m[None, :] * cross_terms / NI


def reference(u_vel, v_vel, u_mask, v_mask, t_mask, bottom, inv_dx, inv_dy):
    level_ids = jnp.arange(K, dtype=jnp.int32)

    def one_level(depth_level_fields):
        return level_flux(depth_level_fields, bottom, inv_dx, inv_dy)

    return lax.map(one_level, (u_vel, v_vel, u_mask, v_mask, t_mask, level_ids)).astype(jnp.float32)
```

```python
import functools

import jax
import jax.numpy as jnp
import numpy as np
from jax import lax
from jax.experimental import pallas as pl
from jax.experimental.pallas import tpu as pltpu
from jax.sharding import PartitionSpec as P

MESH = pl.DeviceIdType.MESH


def up(value, step):
    return -(-value // step) * step


def split_pair(table):
    high = table.astype(jnp.bfloat16)
    low = (table - high.astype(np.float64)).astype(jnp.bfloat16)
    return high, low


class Plan:
    def __init__(self, lon_count, lat_count, levels, rows, cols):
        self.L, self.T, self.K, self.J, self.W = lon_count, lat_count, levels, rows, cols
        self.NI = cols * lon_count
        self.R = rows // lon_count
        best = None
        for n2 in range(2, cols + 1, 2):
            n1 = self.NI // n2
            if cols % n2 or n1 % 4:
                continue
            cost = abs(n1 - 60)
            if best is None or cost < best[0]:
                best = (cost, n2)
        self.N2 = best[1]
        self.N1 = self.NI // self.N2
        self.A = cols // self.N2
        self.AP = up(self.A, 8)
        self.KA = lon_count * self.AP
        self.KO = up(self.N1, 8)
        self.NP = up(self.N2, 8)
        self.PH = self.N2 // 2
        self.U = 4 if self.N2 % 4 == 0 else 2
        self.PO = up(self.PH, 8)
        self.NM = self.NI // 2
        self.WL = up(cols, 128)
        self.WP = up(cols, 8)
        self.B = self.R * levels
        self.LN = up(2 * self.B, 128)
        self.PR = self.AP * self.N2

    def tables(self):
        n = np.arange(self.N2)[:, None, None]
        k = np.arange(self.N1)[None, :, None]
        a = np.arange(self.N1)[None, None, :]
        angle = 2 * np.pi / self.NI * ((k * (self.N2 * a + n)) % self.NI)
        real = np.zeros((self.N2, self.KO, self.L, self.AP))
        imag = np.zeros_like(real)
        real[:, : self.N1, :, : self.A] = np.cos(angle).reshape(self.N2, self.N1, self.L, self.A)
        imag[:, : self.N1, :, : self.A] = -np.sin(angle).reshape(self.N2, self.N1, self.L, self.A)
        first = np.concatenate([real, imag], axis=1).reshape(self.N2, 2 * self.KO, self.KA)
        high, low = split_pair(first)
        first = np.concatenate([high, low], axis=2)
        p = np.arange(self.PH)[:, None]
        m = np.arange(self.N2)[None, :]
        angle = 2 * np.pi / self.N2 * ((p * m) % self.N2)
        second = np.zeros((2, self.PO, 2, self.NP))
        second[0, : self.PH, 0, : self.N2] = np.cos(angle)
        second[0, : self.PH, 1, : self.N2] = np.sin(angle)
        second[1, : self.PH, 0, : self.N2] = -np.sin(angle)
        second[1, : self.PH, 1, : self.N2] = np.cos(angle)
        second = second.reshape(2 * self.PO, 2 * self.NP)
        high, low = split_pair(second)
        second = np.concatenate([high, low, high], axis=1)
        return first, second


def halves(value):
    high = value.astype(jnp.bfloat16)
    low = (value - high.astype(jnp.float32)).astype(jnp.bfloat16)
    return high, low


def kernel(
    p, u_ref, v_ref, um_ref, vm_ref, tm_ref, bot_ref, idx_ref, idy_ref, t1_hbm, t2_ref, out_ref,
    mj, adv, inv, south, north, fold, col_out, col_in, send_a, send_b, got_a, got_b, y_ref,
    f_ref, g_ref, t1, table_sem, halo_send, halo_recv, col_send, col_recv, a_send, a_recv,
    b_send, b_recv,
):
    L, K, J, W, WL = p.L, p.K, p.J, p.W, p.WL
    me = lax.axis_index("lon")
    row = lax.axis_index("lat")
    up_lat, down_lat = lax.rem(row + 1, p.T), lax.rem(row + p.T - 1, p.T)
    right, left = lax.rem(me + 1, L), lax.rem(me + L - 1, L)
    partner = L - 1 - me
    at_north = row == p.T - 1

    table_copy = pltpu.make_async_copy(t1_hbm, t1, table_sem)
    table_copy.start()

    barrier = pltpu.get_barrier_semaphore()
    for off in range(1, L):
        pl.semaphore_signal(
            barrier, inc=1, device_id={"lon": lax.rem(me + off, L)}, device_id_type=MESH
        )
    for other in (up_lat, down_lat):
        pl.semaphore_signal(barrier, inc=1, device_id={"lat": other}, device_id_type=MESH)

    if WL > W:
        tail = jnp.zeros((2, J, K, WL - W), jnp.float32)
        mj[:, :, :, W:] = tail
        adv[:, :, :, W:] = tail
        inv[:, :, W:] = jnp.zeros((2, J, WL - W), jnp.float32)
    inv[0, :, :W] = idx_ref[...] * 0.5
    inv[1, :, :W] = idy_ref[...] * 0.5
    col_out[...] = jnp.zeros_like(col_out)
    for j in range(J):
        mj[0, j, :, :W] = u_ref[:, j, :] * um_ref[:, j, :].astype(jnp.float32)
        mj[1, j, :, :W] = v_ref[:, j, :] * vm_ref[:, j, :].astype(jnp.float32)
    for j in range(J):
        for f in range(2):
            col_out[0, f * K : (f + 1) * K, j : j + 1] = mj[f, j, :, W - 1 : W]
            col_out[1, f * K : (f + 1) * K, j : j + 1] = mj[f, j, :, 0:1]
    pl.semaphore_wait(barrier, L + 1)

    def remote(src, dst, send, recv, device):
        return pltpu.make_async_remote_copy(
            src_ref=src, dst_ref=dst, send_sem=send, recv_sem=recv, device_id=device,
            device_id_type=MESH,
        )

    to_north = remote(mj.at[:, J - 1], south, halo_send.at[0], halo_recv.at[0], {"lat": up_lat})
    to_south = remote(mj.at[:, 0], north, halo_send.at[1], halo_recv.at[1], {"lat": down_lat})
    to_fold = remote(mj.at[:, J - 1], fold, halo_send.at[2], halo_recv.at[2], {"lon": partner})
    to_right = remote(col_out.at[0], col_in.at[0], col_send.at[0], col_recv.at[0], {"lon": right})
    to_left = remote(col_out.at[1], col_in.at[1], col_send.at[1], col_recv.at[1], {"lon": left})
    to_north.start()
    to_south.start()
    to_right.start()
    to_left.start()

    @pl.when(at_north)
    def _():
        to_fold.start()

    def turn(source, target, dest):
        for start in range(0, W, 128):
            pieces = [
                source[f, dest * p.R + r, :, start : start + 128]
                for f in range(2)
                for r in range(p.R)
            ]
            if p.LN > 2 * p.B:
                pieces.append(jnp.zeros((p.LN - 2 * p.B, 128), jnp.float32))
            turned = jnp.transpose(jnp.concatenate(pieces, axis=0))
            size = min(128, p.WP - start)
            target[start : start + size, :] = turned[:size]

    order = sorted(range(1, L), key=lambda off: abs(off - L // 2))

    def exchange(source, buffer, got, send, recv):
        copies = []
        for slot, off in enumerate(order):
            dest = lax.rem(me + off, L)
            turn(source, buffer.at[slot], dest)
            copy = remote(
                buffer.at[slot], got.at[me, pl.ds(0, p.WP)], send.at[slot], recv.at[slot],
                {"lon": dest},
            )
            copy.start()
            copies.append(copy)
        turn(source, got.at[me], me)
        return copies

    if p.PR > p.WP:
        pad = jnp.zeros((L, p.PR - p.WP, p.LN), jnp.float32)
        got_a[:, p.WP :, :] = pad
        got_b[:, p.WP :, :] = pad
    copies_a = exchange(mj, send_a, got_a, a_send, a_recv)

    to_north.wait()
    to_south.wait()
    to_right.wait()
    to_left.wait()

    @pl.when(at_north)
    def _():
        to_fold.wait()
        line = lax.broadcasted_iota(jnp.int32, (128, 128), 0)
        lane = lax.broadcasted_iota(jnp.int32, (128, 128), 1)
        flip = (line + lane == 127).astype(jnp.float32)
        value = fold[...].reshape(2 * K, WL)
        blocks = [
            jnp.dot(
                value[:, start : start + 128], flip, precision=lax.Precision.HIGHEST,
                preferred_element_type=jnp.float32,
            )
            for start in range(WL - 128, -1, -128)
        ]
        turned = jnp.concatenate(blocks, axis=1)
        if WL > W:
            turned = pltpu.roll(turned, W, 1)
        north[...] = -turned.reshape(2, K, WL)

    @pl.when(row == 0)
    def _():
        south[...] = jnp.zeros_like(south)

    lane = lax.broadcasted_iota(jnp.int32, (K, WL), 1)
    level = lax.broadcasted_iota(jnp.int32, (K, W), 0)
    for j in range(J):
        here = [mj[f, j] for f in range(2)]
        inv_x = inv[0, j : j + 1, :]
        inv_y = inv[1, j : j + 1, :]
        live = level < bot_ref[j : j + 1, :]
        weight = jnp.where(live, tm_ref[:, j, :].astype(jnp.float32), 0.0)
        for f in range(2):
            below = south[f] if j == 0 else mj[f, j - 1]
            above = north[f] if j == J - 1 else mj[f, j + 1]
            west = jnp.where(
                lane == 0, col_in[0, f * K : (f + 1) * K, j : j + 1], pltpu.roll(here[f], 1, 1)
            )
            east = jnp.where(
                lane == W - 1, col_in[1, f * K : (f + 1) * K, j : j + 1],
                pltpu.roll(here[f], WL - 1, 1),
            )
            slope_x = (east - west) * inv_x
            slope_y = (above - below) * inv_y
            total = here[0] * slope_x + here[1] * slope_y
            adv[f, j, :, :W] = weight * total[:, :W]

    copies_b = exchange(adv, send_b, got_b, b_send, b_recv)

    if p.NP > p.N2:
        y_ref[p.N2 * 2 * p.KO :, :] = jnp.zeros(
            ((p.NP - p.N2) * 2 * p.KO, p.LN), jnp.float32
        )
    table_copy.wait()

    def first_stage(got):
        def step(block, carry):
            for part in range(p.U):
                n = block * p.U + part
                x = jnp.concatenate(
                    [got[s, pl.ds(n, p.AP, stride=p.N2), :] for s in range(L)], axis=0
                )
                high, low = halves(x)
                data = jnp.concatenate([high, high, low, low], axis=0)
                table = t1[n]
                out = jnp.dot(
                    jnp.concatenate([table, table], axis=1), data,
                    preferred_element_type=jnp.float32,
                )
                y_ref[pl.ds(pl.multiple_of(n * 2 * p.KO, 8), 2 * p.KO), :] = out
            return carry

        lax.fori_loop(0, p.N2 // p.U, step, 0)

    def second_stage(finish):
        table = t2_ref[...]

        def step(block, carry):
            for part in range(2):
                ks = [block * 4 + part * 2 + q for q in range(2)]
                sides = []
                for k in ks:
                    y = jnp.concatenate(
                        [
                            y_ref[pl.ds(k + c * p.KO, p.NP, stride=2 * p.KO), :]
                            for c in range(2)
                        ],
                        axis=0,
                    )
                    high, low = halves(y)
                    sides.append(jnp.concatenate([high, high, low], axis=0))
                out = jnp.dot(
                    table, jnp.concatenate(sides, axis=1), preferred_element_type=jnp.float32
                )
                for q, k in enumerate(ks):
                    finish(k, out[:, q * p.LN : (q + 1) * p.LN])
            return carry

        lax.fori_loop(0, p.N1 // 4, step, 0)

    def keep(k, value):
        f_ref[k] = value

    def cross(k, value):
        both = f_ref[k] * value
        g_ref[pl.ds(k, p.PO, stride=p.N1), :] = both[: p.PO] + both[p.PO :]

    for copy in copies_a:
        copy.wait()
    first_stage(got_a)
    second_stage(keep)
    for copy in copies_b:
        copy.wait()
    first_stage(got_b)
    second_stage(cross)

    for start in range(0, p.NM, 128):
        size = min(128, p.NM - start)
        block = jnp.transpose(g_ref[start : start + 128, :])
        wave = lax.broadcasted_iota(jnp.int32, (p.B, 128), 1) + start
        scale = jnp.where(wave == 0, -1.0 / p.NI, -2.0 / p.NI)
        total = (block[: p.B] + block[p.B : 2 * p.B]) * scale
        out_ref[:, start : start + size] = total[:, :size]


def body(p, *args):
    first, second = p.tables()
    f32 = jnp.float32
    vmem = pl.BlockSpec(memory_space=pltpu.VMEM)
    dma = pltpu.SemaphoreType.DMA
    out = pl.pallas_call(
        functools.partial(kernel, p),
        out_shape=jax.ShapeDtypeStruct((p.B, p.NM), f32),
        in_specs=[vmem] * 8 + [pl.BlockSpec(memory_space=pl.ANY), vmem],
        out_specs=vmem,
        scratch_shapes=[
            pltpu.VMEM((2, p.J, p.K, p.WL), f32),
            pltpu.VMEM((2, p.J, p.K, p.WL), f32),
            pltpu.VMEM((2, p.J, p.WL), f32),
            pltpu.VMEM((2, p.K, p.WL), f32),
            pltpu.VMEM((2, p.K, p.WL), f32),
            pltpu.VMEM((2, p.K, p.WL), f32),
            pltpu.VMEM((2, 2 * p.K, 128), f32),
            pltpu.VMEM((2, 2 * p.K, 128), f32),
            pltpu.VMEM((p.L - 1, p.WP, p.LN), f32),
            pltpu.VMEM((p.L - 1, p.WP, p.LN), f32),
            pltpu.VMEM((p.L, p.PR, p.LN), f32),
            pltpu.VMEM((p.L, p.PR, p.LN), f32),
            pltpu.VMEM((p.NP * 2 * p.KO, p.LN), f32),
            pltpu.VMEM((p.N1, 2 * p.PO, p.LN), f32),
            pltpu.VMEM((max(p.PO * p.N1, up(p.NM, 128)), p.LN), f32),
            pltpu.VMEM((p.N2, 2 * p.KO, 2 * p.KA), jnp.bfloat16),
            dma(()),
            dma((3,)),
            dma((3,)),
            dma((2,)),
            dma((2,)),
            dma((p.L - 1,)),
            dma((p.L - 1,)),
            dma((p.L - 1,)),
            dma((p.L - 1,)),
        ],
        compiler_params=pltpu.CompilerParams(
            collective_id=0, has_side_effects=True, vmem_limit_bytes=62 * 1024 * 1024
        ),
    )(*args, jnp.asarray(first), jnp.asarray(second))
    return jnp.transpose(out.reshape(p.R, p.K, p.NM), (1, 0, 2))


def solution(mesh):
    field = P(None, "lat", "lon")
    flat = P("lat", "lon")

    def run(*args):
        levels, rows, cols = args[0].shape
        plan = Plan(mesh.shape["lon"], mesh.shape["lat"], levels, rows, cols)
        return body(plan, *args)

    return jax.shard_map(
        run, mesh=mesh, in_specs=(field,) * 5 + (flat,) * 3,
        out_specs=P(None, ("lat", "lon"), None), check_vma=False,
    )
```

```python
import functools

import jax
import jax.numpy as jnp
import numpy as np
from jax import lax
from jax.experimental import pallas as pl
from jax.experimental.pallas import tpu as pltpu
from jax.sharding import PartitionSpec as P

MESH = pl.DeviceIdType.MESH


def up(value, step):
    return -(-value // step) * step


def split_pair(table):
    high = table.astype(jnp.bfloat16)
    low = (table - high.astype(np.float64)).astype(jnp.bfloat16)
    return high, low


class Plan:
    def __init__(self, lon_count, lat_count, levels, rows, cols):
        self.L, self.T, self.K, self.J, self.W = lon_count, lat_count, levels, rows, cols
        self.NI = cols * lon_count
        self.R = rows // lon_count
        best = None
        for n2 in range(2, cols + 1, 2):
            n1 = self.NI // n2
            if cols % n2 or n1 % 4:
                continue
            cost = abs(n1 - 60)
            if best is None or cost < best[0]:
                best = (cost, n2)
        self.N2 = best[1]
        self.N1 = self.NI // self.N2
        self.A = cols // self.N2
        self.AP = up(self.A, 8)
        self.KA = lon_count * self.AP
        self.KO = up(self.N1, 8)
        self.NP = up(self.N2, 8)
        self.PH = self.N2 // 2
        self.C = 3 if self.N2 % 24 == 0 and cols % 8 == 0 else 1
        self.U = 4 if self.N2 % 4 == 0 else 2
        self.PO = up(self.PH, 8)
        self.NM = self.NI // 2
        self.WL = up(cols, 128)
        self.WP = up(cols, 8)
        self.B = self.R * levels
        self.LN = up(2 * self.B, 128)
        self.PR = self.AP * self.N2

    def tables(self):
        n = np.arange(self.N2)[:, None, None]
        k = np.arange(self.N1)[None, :, None]
        a = np.arange(self.N1)[None, None, :]
        angle = 2 * np.pi / self.NI * ((k * (self.N2 * a + n)) % self.NI)
        real = np.zeros((self.N2, self.KO, self.L, self.AP))
        imag = np.zeros_like(real)
        real[:, : self.N1, :, : self.A] = np.cos(angle).reshape(self.N2, self.N1, self.L, self.A)
        imag[:, : self.N1, :, : self.A] = -np.sin(angle).reshape(self.N2, self.N1, self.L, self.A)
        first = np.concatenate([real, imag], axis=1).reshape(self.N2, 2 * self.KO, self.KA)
        high, low = split_pair(first)
        first = np.concatenate([high, low], axis=2)
        p = np.arange(self.PH)[:, None]
        m = np.arange(self.N2)[None, :]
        angle = 2 * np.pi / self.N2 * ((p * m) % self.N2)
        second = np.zeros((2, self.PO, 2, self.NP))
        second[0, : self.PH, 0, : self.N2] = np.cos(angle)
        second[0, : self.PH, 1, : self.N2] = np.sin(angle)
        second[1, : self.PH, 0, : self.N2] = -np.sin(angle)
        second[1, : self.PH, 1, : self.N2] = np.cos(angle)
        second = second.reshape(2 * self.PO, 2 * self.NP)
        high, low = split_pair(second)
        second = np.concatenate([high, low, high], axis=1)
        return first, second


def halves(value):
    high = value.astype(jnp.bfloat16)
    low = (value - high.astype(jnp.float32)).astype(jnp.bfloat16)
    return high, low


def kernel(
    p, u_ref, v_ref, um_ref, vm_ref, tm_ref, bot_ref, idx_ref, idy_ref, t1_hbm, t2_ref, out_ref,
    mj, adv, inv, south, north, fold, col_out, col_in, send_a, send_b, got_a, got_b, y_ref,
    f_ref, g_ref, turned_out, t1, table_sem, halo_send, halo_recv, col_send, col_recv, a_send, a_recv,
    b_send, b_recv,
):
    L, K, J, W, WL = p.L, p.K, p.J, p.W, p.WL
    me = lax.axis_index("lon")
    row = lax.axis_index("lat")
    up_lat, down_lat = lax.rem(row + 1, p.T), lax.rem(row + p.T - 1, p.T)
    right, left = lax.rem(me + 1, L), lax.rem(me + L - 1, L)
    partner = L - 1 - me
    at_north = row == p.T - 1

    table_copy = pltpu.make_async_copy(t1_hbm, t1, table_sem)
    table_copy.start()

    barrier = pltpu.get_barrier_semaphore()
    for off in range(1, L):
        pl.semaphore_signal(
            barrier, inc=1, device_id={"lon": lax.rem(me + off, L)}, device_id_type=MESH
        )
    for other in (up_lat, down_lat):
        pl.semaphore_signal(barrier, inc=1, device_id={"lat": other}, device_id_type=MESH)

    if WL > W:
        tail = jnp.zeros((2, J, K, WL - W), jnp.float32)
        mj[:, :, :, W:] = tail
        adv[:, :, :, W:] = tail
        inv[:, :, W:] = jnp.zeros((2, J, WL - W), jnp.float32)
    inv[0, :, :W] = idx_ref[...] * 0.5
    inv[1, :, :W] = idy_ref[...] * 0.5
    col_out[...] = jnp.zeros_like(col_out)
    for j in range(J):
        mj[0, j, :, :W] = u_ref[:, j, :] * um_ref[:, j, :].astype(jnp.float32)
        mj[1, j, :, :W] = v_ref[:, j, :] * vm_ref[:, j, :].astype(jnp.float32)
    for j in range(J):
        for f in range(2):
            col_out[0, f * K : (f + 1) * K, j : j + 1] = mj[f, j, :, W - 1 : W]
            col_out[1, f * K : (f + 1) * K, j : j + 1] = mj[f, j, :, 0:1]
    pl.semaphore_wait(barrier, L + 1)

    def remote(src, dst, send, recv, device):
        return pltpu.make_async_remote_copy(
            src_ref=src, dst_ref=dst, send_sem=send, recv_sem=recv, device_id=device,
            device_id_type=MESH,
        )

    to_north = remote(mj.at[:, J - 1], south, halo_send.at[0], halo_recv.at[0], {"lat": up_lat})
    to_south = remote(mj.at[:, 0], north, halo_send.at[1], halo_recv.at[1], {"lat": down_lat})
    to_fold = remote(mj.at[:, J - 1], fold, halo_send.at[2], halo_recv.at[2], {"lon": partner})
    to_right = remote(col_out.at[0], col_in.at[0], col_send.at[0], col_recv.at[0], {"lon": right})
    to_left = remote(col_out.at[1], col_in.at[1], col_send.at[1], col_recv.at[1], {"lon": left})
    to_north.start()
    to_south.start()
    to_right.start()
    to_left.start()

    @pl.when(at_north)
    def _():
        to_fold.start()

    def turn(source, target, dest):
        for start in range(0, W, 128):
            pieces = [
                source[f, dest * p.R + r, :, start : start + 128]
                for f in range(2)
                for r in range(p.R)
            ]
            if p.LN > 2 * p.B:
                pieces.append(jnp.zeros((p.LN - 2 * p.B, 128), jnp.float32))
            turned = jnp.transpose(jnp.concatenate(pieces, axis=0))
            size = min(128, p.WP - start)
            target[start : start + size, :] = turned[:size]

    order = sorted(range(1, L), key=lambda off: abs(off - L // 2))

    def exchange(source, buffer, got, send, recv, chunks):
        copies = [[] for _ in range(chunks)]
        width = p.N2 // chunks
        for slot, off in enumerate(order):
            dest = lax.rem(me + off, L)
            turn(source, buffer.at[slot], dest)
            for c in range(chunks):
                if chunks == 1:
                    src, dst = buffer.at[slot], got.at[me, pl.ds(0, p.WP)]
                else:
                    part = pl.ds(c * width, width)
                    src = buffer.at[slot].reshape(p.A, p.N2, p.LN).at[:, part]
                    dst = got.at[me].reshape(p.AP, p.N2, p.LN).at[pl.ds(0, p.A), part]
                copies[c].append(
                    remote(src, dst, send.at[c, slot], recv.at[c, slot], {"lon": dest})
                )
                if c == 0:
                    copies[c][-1].start()
        for group in copies[1:]:
            for copy in group:
                copy.start()
        turn(source, got.at[me], me)
        return copies

    if p.PR > p.WP:
        pad = jnp.zeros((L, p.PR - p.WP, p.LN), jnp.float32)
        got_a[:, p.WP :, :] = pad
        got_b[:, p.WP :, :] = pad
    copies_a = exchange(mj, send_a, got_a, a_send, a_recv, 1)

    to_north.wait()
    to_south.wait()
    to_right.wait()
    to_left.wait()

    @pl.when(at_north)
    def _():
        to_fold.wait()
        line = lax.broadcasted_iota(jnp.int32, (128, 128), 0)
        lane = lax.broadcasted_iota(jnp.int32, (128, 128), 1)
        flip = (line + lane == 127).astype(jnp.float32)
        value = fold[...].reshape(2 * K, WL)
        blocks = [
            jnp.dot(
                value[:, start : start + 128], flip, precision=lax.Precision.HIGHEST,
                preferred_element_type=jnp.float32,
            )
            for start in range(WL - 128, -1, -128)
        ]
        turned = jnp.concatenate(blocks, axis=1)
        if WL > W:
            turned = pltpu.roll(turned, W, 1)
        north[...] = -turned.reshape(2, K, WL)

    @pl.when(row == 0)
    def _():
        south[...] = jnp.zeros_like(south)

    lane = lax.broadcasted_iota(jnp.int32, (K, WL), 1)
    level = lax.broadcasted_iota(jnp.int32, (K, W), 0)
    for j in range(J):
        here = [mj[f, j] for f in range(2)]
        inv_x = inv[0, j : j + 1, :]
        inv_y = inv[1, j : j + 1, :]
        live = level < bot_ref[j : j + 1, :]
        weight = jnp.where(live, tm_ref[:, j, :].astype(jnp.float32), 0.0)
        for f in range(2):
            below = south[f] if j == 0 else mj[f, j - 1]
            above = north[f] if j == J - 1 else mj[f, j + 1]
            west = jnp.where(
                lane == 0, col_in[0, f * K : (f + 1) * K, j : j + 1], pltpu.roll(here[f], 1, 1)
            )
            east = jnp.where(
                lane == W - 1, col_in[1, f * K : (f + 1) * K, j : j + 1],
                pltpu.roll(here[f], WL - 1, 1),
            )
            slope_x = (east - west) * inv_x
            slope_y = (above - below) * inv_y
            total = here[0] * slope_x + here[1] * slope_y
            adv[f, j, :, :W] = weight * total[:, :W]

    copies_b = exchange(adv, send_b, got_b, b_send, b_recv, p.C)

    if p.NP > p.N2:
        y_ref[p.N2 * 2 * p.KO :, :] = jnp.zeros(
            ((p.NP - p.N2) * 2 * p.KO, p.LN), jnp.float32
        )
    table_copy.wait()

    def first_stage(got, c=0, chunks=1):
        size = p.N2 // chunks // p.U

        def step(block, carry):
            for part in range(p.U):
                n = block * p.U + part
                x = jnp.concatenate(
                    [got[s, pl.ds(n, p.AP, stride=p.N2), :] for s in range(L)], axis=0
                )
                high, low = halves(x)
                data = jnp.concatenate([high, high, low, low], axis=0)
                table = t1[n]
                out = jnp.dot(
                    jnp.concatenate([table, table], axis=1), data,
                    preferred_element_type=jnp.float32,
                )
                y_ref[pl.ds(pl.multiple_of(n * 2 * p.KO, 8), 2 * p.KO), :] = out
            return carry

        lax.fori_loop(c * size, (c + 1) * size, step, 0)

    def second_stage(finish):
        table = t2_ref[...]

        def step(block, carry):
            for part in range(2):
                ks = [block * 4 + part * 2 + q for q in range(2)]
                sides = []
                for k in ks:
                    y = jnp.concatenate(
                        [
                            y_ref[pl.ds(k + c * p.KO, p.NP, stride=2 * p.KO), :]
                            for c in range(2)
                        ],
                        axis=0,
                    )
                    high, low = halves(y)
                    sides.append(jnp.concatenate([high, high, low], axis=0))
                out = jnp.dot(
                    table, jnp.concatenate(sides, axis=1), preferred_element_type=jnp.float32
                )
                for q, k in enumerate(ks):
                    finish(k, out[:, q * p.LN : (q + 1) * p.LN])
            return carry

        lax.fori_loop(0, p.N1 // 4, step, 0)

    def keep(k, value):
        f_ref[k] = value

    def cross(k, value):
        both = f_ref[k] * value
        g_ref[pl.ds(k, p.PO, stride=p.N1), :] = both[: p.PO] + both[p.PO :]

    for copy in copies_a[0]:
        copy.wait()
    first_stage(got_a)
    second_stage(keep)
    for c, group in enumerate(copies_b):
        for copy in group:
            copy.wait()
        first_stage(got_b, c, p.C)
    second_stage(cross)

    for start in range(0, p.NM, 128):
        size = min(128, p.NM - start)
        block = jnp.transpose(g_ref[start : start + 128, :])
        wave = lax.broadcasted_iota(jnp.int32, (p.B, 128), 1) + start
        scale = jnp.where(wave == 0, -1.0 / p.NI, -2.0 / p.NI)
        total = (block[: p.B] + block[p.B : 2 * p.B]) * scale
        turned_out[start // 128] = total
        for k in range(p.K):
            rows = turned_out[start // 128, pl.ds(k, p.R, stride=p.K), :]
            out_ref[k, :, start : start + size] = rows[:, :size]


def body(p, *args):
    first, second = p.tables()
    f32 = jnp.float32
    vmem = pl.BlockSpec(memory_space=pltpu.VMEM)
    dma = pltpu.SemaphoreType.DMA
    return pl.pallas_call(
        functools.partial(kernel, p),
        out_shape=jax.ShapeDtypeStruct((p.K, p.R, p.NM), f32),
        in_specs=[vmem] * 8 + [pl.BlockSpec(memory_space=pl.ANY), vmem],
        out_specs=vmem,
        scratch_shapes=[
            pltpu.VMEM((2, p.J, p.K, p.WL), f32),
            pltpu.VMEM((2, p.J, p.K, p.WL), f32),
            pltpu.VMEM((2, p.J, p.WL), f32),
            pltpu.VMEM((2, p.K, p.WL), f32),
            pltpu.VMEM((2, p.K, p.WL), f32),
            pltpu.VMEM((2, p.K, p.WL), f32),
            pltpu.VMEM((2, 2 * p.K, 128), f32),
            pltpu.VMEM((2, 2 * p.K, 128), f32),
            pltpu.VMEM((p.L - 1, p.WP, p.LN), f32),
            pltpu.VMEM((p.L - 1, p.WP, p.LN), f32),
            pltpu.VMEM((p.L, p.PR, p.LN), f32),
            pltpu.VMEM((p.L, p.PR, p.LN), f32),
            pltpu.VMEM((p.NP * 2 * p.KO, p.LN), f32),
            pltpu.VMEM((p.N1, 2 * p.PO, p.LN), f32),
            pltpu.VMEM((max(p.PO * p.N1, up(p.NM, 128)), p.LN), f32),
            pltpu.VMEM((up(p.NM, 128) // 128, p.B, 128), f32),
            pltpu.VMEM((p.N2, 2 * p.KO, 2 * p.KA), jnp.bfloat16),
            dma(()),
            dma((3,)),
            dma((3,)),
            dma((2,)),
            dma((2,)),
            dma((1, p.L - 1)),
            dma((1, p.L - 1)),
            dma((p.C, p.L - 1)),
            dma((p.C, p.L - 1)),
        ],
        compiler_params=pltpu.CompilerParams(
            collective_id=0, has_side_effects=True, vmem_limit_bytes=62 * 1024 * 1024
        ),
    )(*args, jnp.asarray(first), jnp.asarray(second))


def solution(mesh):
    field = P(None, "lat", "lon")
    flat = P("lat", "lon")

    def run(*args):
        levels, rows, cols = args[0].shape
        plan = Plan(mesh.shape["lon"], mesh.shape["lat"], levels, rows, cols)
        return body(plan, *args)

    return jax.shard_map(
        run, mesh=mesh, in_specs=(field,) * 5 + (flat,) * 3,
        out_specs=P(None, ("lat", "lon"), None), check_vma=False,
    )
```

```python
import functools

import jax
import jax.numpy as jnp
import numpy as np
from jax import lax
from jax.experimental import pallas as pl
from jax.experimental.pallas import tpu as pltpu
from jax.sharding import PartitionSpec as P

MESH = pl.DeviceIdType.MESH


def up(value, step):
    return -(-value // step) * step


def split_pair(table):
    high = table.astype(jnp.bfloat16)
    low = (table - high.astype(np.float64)).astype(jnp.bfloat16)
    return high, low


class Plan:
    def __init__(self, lon_count, lat_count, levels, rows, cols):
        self.L, self.T, self.K, self.J, self.W = lon_count, lat_count, levels, rows, cols
        self.NI = cols * lon_count
        self.R = rows // lon_count
        best = None
        for n2 in range(2, cols + 1, 2):
            n1 = self.NI // n2
            if cols % n2 or n1 % 4:
                continue
            cost = abs(n1 - 60)
            if best is None or cost < best[0]:
                best = (cost, n2)
        self.N2 = best[1]
        self.N1 = self.NI // self.N2
        self.A = cols // self.N2
        self.AP = up(self.A, 8)
        self.KA = lon_count * self.AP
        self.KO = up(self.N1, 8)
        self.NP = up(self.N2, 8)
        self.PH = self.N2 // 2
        self.parts = [self.N2]
        if self.N2 % 8 == 0 and cols % 8 == 0 and self.N2 >= 48:
            self.parts = [self.N2 - 24, 16, 8]
        self.C = len(self.parts)
        self.starts = [sum(self.parts[:c]) for c in range(self.C)]
        self.U = 4 if self.N2 % 4 == 0 else 2
        self.PO = up(self.PH, 8)
        self.NM = self.NI // 2
        self.WL = up(cols, 128)
        self.WP = up(cols, 8)
        self.B = self.R * levels
        self.LN = up(2 * self.B, 128)
        self.PR = self.AP * self.N2

    def tables(self):
        n = np.arange(self.N2)[:, None, None]
        k = np.arange(self.N1)[None, :, None]
        a = np.arange(self.N1)[None, None, :]
        angle = 2 * np.pi / self.NI * ((k * (self.N2 * a + n)) % self.NI)
        real = np.zeros((self.N2, self.KO, self.L, self.AP))
        imag = np.zeros_like(real)
        real[:, : self.N1, :, : self.A] = np.cos(angle).reshape(self.N2, self.N1, self.L, self.A)
        imag[:, : self.N1, :, : self.A] = -np.sin(angle).reshape(self.N2, self.N1, self.L, self.A)
        first = np.concatenate([real, imag], axis=1).reshape(self.N2, 2 * self.KO, self.KA)
        high, low = split_pair(first)
        first = np.concatenate([high, low], axis=2)
        p = np.arange(self.PH)[:, None]
        m = np.arange(self.N2)[None, :]
        angle = 2 * np.pi / self.N2 * ((p * m) % self.N2)
        second = np.zeros((2, self.PO, 2, self.NP))
        second[0, : self.PH, 0, : self.N2] = np.cos(angle)
        second[0, : self.PH, 1, : self.N2] = np.sin(angle)
        second[1, : self.PH, 0, : self.N2] = -np.sin(angle)
        second[1, : self.PH, 1, : self.N2] = np.cos(angle)
        pieces = []
        for start, size in self.spans():
            piece = second[:, :, :, start : start + size].reshape(2 * self.PO, 2 * size)
            high, low = split_pair(piece)
            piece = np.concatenate([high, low, high], axis=1)
            pieces.append(np.pad(piece, ((0, 0), (0, up(6 * size, 128) - 6 * size))))
        return first, np.concatenate(pieces, axis=1)

    def spans(self):
        every = [(0, self.NP)]
        if self.C > 1:
            every += list(zip(self.starts, self.parts))
        return every

    def span(self, index):
        start, size = self.spans()[index]
        before = sum(up(6 * width, 128) for _, width in self.spans()[:index])
        return start, size, before


def halves(value):
    high = value.astype(jnp.bfloat16)
    low = (value - high.astype(jnp.float32)).astype(jnp.bfloat16)
    return high, low


def kernel(
    p, u_hbm, v_hbm, um_hbm, vm_hbm, tm_hbm, bot_ref, idx_ref, idy_ref, t1_hbm, t2_ref, out_ref,
    mj, adv, inv, south, north, fold, col_out, col_in, send_a, send_b, got_a, got_b, y_ref,
    f_ref, p_ref, g_ref, turned_out, u_ref, v_ref, um_ref, vm_ref, tm_ref, t1, in_sem, table_sem, halo_send, halo_recv, col_send, col_recv, a_send, a_recv,
    b_send, b_recv,
):
    L, K, J, W, WL = p.L, p.K, p.J, p.W, p.WL
    me = lax.axis_index("lon")
    row = lax.axis_index("lat")
    up_lat, down_lat = lax.rem(row + 1, p.T), lax.rem(row + p.T - 1, p.T)
    right, left = lax.rem(me + 1, L), lax.rem(me + L - 1, L)
    partner = L - 1 - me
    at_north = row == p.T - 1

    loads = [
        pltpu.make_async_copy(src, dst, in_sem.at[at])
        for at, (src, dst) in enumerate(
            [(u_hbm, u_ref), (um_hbm, um_ref), (v_hbm, v_ref), (vm_hbm, vm_ref), (tm_hbm, tm_ref)]
        )
    ]
    for load in loads:
        load.start()
    table_copy = pltpu.make_async_copy(t1_hbm, t1, table_sem)
    table_copy.start()

    barrier = pltpu.get_barrier_semaphore()
    for off in range(1, L):
        pl.semaphore_signal(
            barrier, inc=1, device_id={"lon": lax.rem(me + off, L)}, device_id_type=MESH
        )
    for other in (up_lat, down_lat):
        pl.semaphore_signal(barrier, inc=1, device_id={"lat": other}, device_id_type=MESH)

    if WL > W:
        tail = jnp.zeros((2, J, K, WL - W), jnp.float32)
        mj[:, :, :, W:] = tail
        adv[:, :, :, W:] = tail
        inv[:, :, W:] = jnp.zeros((2, J, WL - W), jnp.float32)
    inv[0, :, :W] = idx_ref[...] * 0.5
    inv[1, :, :W] = idy_ref[...] * 0.5
    col_out[...] = jnp.zeros_like(col_out)
    for load in loads[:2]:
        load.wait()
    for j in range(J):
        mj[0, j, :, :W] = u_ref[:, j, :] * um_ref[:, j, :].astype(jnp.float32)
    for load in loads[2:4]:
        load.wait()
    for j in range(J):
        mj[1, j, :, :W] = v_ref[:, j, :] * vm_ref[:, j, :].astype(jnp.float32)
    for j in range(J):
        for f in range(2):
            col_out[0, f * K : (f + 1) * K, j : j + 1] = mj[f, j, :, W - 1 : W]
            col_out[1, f * K : (f + 1) * K, j : j + 1] = mj[f, j, :, 0:1]
    pl.semaphore_wait(barrier, L + 1)

    def remote(src, dst, send, recv, device):
        return pltpu.make_async_remote_copy(
            src_ref=src, dst_ref=dst, send_sem=send, recv_sem=recv, device_id=device,
            device_id_type=MESH,
        )

    to_north = remote(mj.at[:, J - 1], south, halo_send.at[0], halo_recv.at[0], {"lat": up_lat})
    to_south = remote(mj.at[:, 0], north, halo_send.at[1], halo_recv.at[1], {"lat": down_lat})
    to_fold = remote(mj.at[:, J - 1], fold, halo_send.at[2], halo_recv.at[2], {"lon": partner})
    to_right = remote(col_out.at[0], col_in.at[0], col_send.at[0], col_recv.at[0], {"lon": right})
    to_left = remote(col_out.at[1], col_in.at[1], col_send.at[1], col_recv.at[1], {"lon": left})
    to_north.start()
    to_south.start()
    to_right.start()
    to_left.start()

    @pl.when(at_north)
    def _():
        to_fold.start()

    def turn(source, target, dest):
        for start in range(0, W, 128):
            pieces = [
                source[f, dest * p.R + r, :, start : start + 128]
                for f in range(2)
                for r in range(p.R)
            ]
            if p.LN > 2 * p.B:
                pieces.append(jnp.zeros((p.LN - 2 * p.B, 128), jnp.float32))
            turned = jnp.transpose(jnp.concatenate(pieces, axis=0))
            size = min(128, p.WP - start)
            target[start : start + size, :] = turned[:size]

    order = sorted(range(1, L), key=lambda off: abs(off - L // 2))

    def exchange(source, buffer, got, send, recv, chunks):
        copies = [[] for _ in range(chunks)]
        for slot, off in enumerate(order):
            dest = lax.rem(me + off, L)
            turn(source, buffer.at[slot], dest)
            for c in range(chunks):
                if chunks == 1:
                    src, dst = buffer.at[slot], got.at[me, pl.ds(0, p.WP)]
                else:
                    part = pl.ds(p.starts[c], p.parts[c])
                    src = buffer.at[slot].reshape(p.A, p.N2, p.LN).at[:, part]
                    dst = got.at[me].reshape(p.AP, p.N2, p.LN).at[pl.ds(0, p.A), part]
                copies[c].append(
                    remote(src, dst, send.at[c, slot], recv.at[c, slot], {"lon": dest})
                )
                if c == 0:
                    copies[c][-1].start()
        for group in copies[1:]:
            for copy in group:
                copy.start()
        turn(source, got.at[me], me)
        return copies

    if p.PR > p.WP:
        pad = jnp.zeros((L, p.PR - p.WP, p.LN), jnp.float32)
        got_a[:, p.WP :, :] = pad
        got_b[:, p.WP :, :] = pad
    copies_a = exchange(mj, send_a, got_a, a_send, a_recv, 1)

    to_north.wait()
    to_south.wait()
    to_right.wait()
    to_left.wait()

    @pl.when(at_north)
    def _():
        to_fold.wait()
        line = lax.broadcasted_iota(jnp.int32, (128, 128), 0)
        lane = lax.broadcasted_iota(jnp.int32, (128, 128), 1)
        flip = (line + lane == 127).astype(jnp.float32)
        value = fold[...].reshape(2 * K, WL)
        blocks = [
            jnp.dot(
                value[:, start : start + 128], flip, precision=lax.Precision.HIGHEST,
                preferred_element_type=jnp.float32,
            )
            for start in range(WL - 128, -1, -128)
        ]
        turned = jnp.concatenate(blocks, axis=1)
        if WL > W:
            turned = pltpu.roll(turned, W, 1)
        north[...] = -turned.reshape(2, K, WL)

    @pl.when(row == 0)
    def _():
        south[...] = jnp.zeros_like(south)

    loads[4].wait()
    lane = lax.broadcasted_iota(jnp.int32, (K, WL), 1)
    level = lax.broadcasted_iota(jnp.int32, (K, W), 0)
    for j in range(J):
        here = [mj[f, j] for f in range(2)]
        inv_x = inv[0, j : j + 1, :]
        inv_y = inv[1, j : j + 1, :]
        live = level < bot_ref[j : j + 1, :]
        weight = jnp.where(live, tm_ref[:, j, :].astype(jnp.float32), 0.0)
        for f in range(2):
            below = south[f] if j == 0 else mj[f, j - 1]
            above = north[f] if j == J - 1 else mj[f, j + 1]
            west = jnp.where(
                lane == 0, col_in[0, f * K : (f + 1) * K, j : j + 1], pltpu.roll(here[f], 1, 1)
            )
            east = jnp.where(
                lane == W - 1, col_in[1, f * K : (f + 1) * K, j : j + 1],
                pltpu.roll(here[f], WL - 1, 1),
            )
            slope_x = (east - west) * inv_x
            slope_y = (above - below) * inv_y
            total = here[0] * slope_x + here[1] * slope_y
            adv[f, j, :, :W] = weight * total[:, :W]

    copies_b = exchange(adv, send_b, got_b, b_send, b_recv, p.C)

    if p.NP > p.N2:
        y_ref[p.N2 * 2 * p.KO :, :] = jnp.zeros(
            ((p.NP - p.N2) * 2 * p.KO, p.LN), jnp.float32
        )
    table_copy.wait()

    def first_stage(got, begin, end):

        def step(block, carry):
            for part in range(p.U):
                n = block * p.U + part
                x = jnp.concatenate(
                    [got[s, pl.ds(n, p.AP, stride=p.N2), :] for s in range(L)], axis=0
                )
                high, low = halves(x)
                data = jnp.concatenate([high, high, low, low], axis=0)
                table = t1[n]
                out = jnp.dot(
                    jnp.concatenate([table, table], axis=1), data,
                    preferred_element_type=jnp.float32,
                )
                y_ref[pl.ds(pl.multiple_of(n * 2 * p.KO, 8), 2 * p.KO), :] = out
            return carry

        lax.fori_loop(begin // p.U, end // p.U, step, 0)

    def second_stage(finish, index):
        begin, size, before = p.span(index)
        table = t2_ref[:, before : before + 6 * size]

        def step(block, carry):
            for part in range(2):
                ks = [block * 4 + part * 2 + q for q in range(2)]
                sides = []
                for k in ks:
                    y = jnp.concatenate(
                        [
                            y_ref[pl.ds(2 * p.KO * begin + k + c * p.KO, size, stride=2 * p.KO), :]
                            for c in range(2)
                        ],
                        axis=0,
                    )
                    high, low = halves(y)
                    sides.append(jnp.concatenate([high, high, low], axis=0))
                out = jnp.dot(
                    table, jnp.concatenate(sides, axis=1), preferred_element_type=jnp.float32
                )
                for q, k in enumerate(ks):
                    finish(k, out[:, q * p.LN : (q + 1) * p.LN])
            return carry

        lax.fori_loop(0, p.N1 // 4, step, 0)

    def keep(k, value):
        f_ref[k] = value

    def begin_sum(k, value):
        p_ref[k] = value

    def add_sum(k, value):
        p_ref[k] += value

    def cross(k, value):
        both = f_ref[k] * (value if p.C == 1 else p_ref[k] + value)
        g_ref[pl.ds(k, p.PO, stride=p.N1), :] = both[: p.PO] + both[p.PO :]

    for copy in copies_a[0]:
        copy.wait()
    first_stage(got_a, 0, p.N2)
    second_stage(keep, 0)
    for c, group in enumerate(copies_b):
        for copy in group:
            copy.wait()
        first_stage(got_b, p.starts[c], p.starts[c] + p.parts[c])
        finish = cross if c == p.C - 1 else begin_sum if c == 0 else add_sum
        second_stage(finish, c + 1 if p.C > 1 else 0)

    for start in range(0, p.NM, 128):
        size = min(128, p.NM - start)
        block = jnp.transpose(g_ref[start : start + 128, :])
        wave = lax.broadcasted_iota(jnp.int32, (p.B, 128), 1) + start
        scale = jnp.where(wave == 0, -1.0 / p.NI, -2.0 / p.NI)
        total = (block[: p.B] + block[p.B : 2 * p.B]) * scale
        turned_out[start // 128] = total
        for k in range(p.K):
            rows = turned_out[start // 128, pl.ds(k, p.R, stride=p.K), :]
            out_ref[k, :, start : start + size] = rows[:, :size]


def body(p, *args):
    first, second = p.tables()
    f32 = jnp.float32
    vmem = pl.BlockSpec(memory_space=pltpu.VMEM)
    hbm = pl.BlockSpec(memory_space=pl.ANY)
    dma = pltpu.SemaphoreType.DMA
    block = (p.K, p.J, p.W)
    return pl.pallas_call(
        functools.partial(kernel, p),
        out_shape=jax.ShapeDtypeStruct((p.K, p.R, p.NM), f32),
        in_specs=[hbm] * 5 + [vmem] * 3 + [hbm, vmem],
        out_specs=vmem,
        scratch_shapes=[
            pltpu.VMEM((2, p.J, p.K, p.WL), f32),
            pltpu.VMEM((2, p.J, p.K, p.WL), f32),
            pltpu.VMEM((2, p.J, p.WL), f32),
            pltpu.VMEM((2, p.K, p.WL), f32),
            pltpu.VMEM((2, p.K, p.WL), f32),
            pltpu.VMEM((2, p.K, p.WL), f32),
            pltpu.VMEM((2, 2 * p.K, 128), f32),
            pltpu.VMEM((2, 2 * p.K, 128), f32),
            pltpu.VMEM((p.L - 1, p.WP, p.LN), f32),
            pltpu.VMEM((p.L - 1, p.WP, p.LN), f32),
            pltpu.VMEM((p.L, p.PR, p.LN), f32),
            pltpu.VMEM((p.L, p.PR, p.LN), f32),
            pltpu.VMEM((p.NP * 2 * p.KO, p.LN), f32),
            pltpu.VMEM((p.N1, 2 * p.PO, p.LN), f32),
            pltpu.VMEM((p.N1, 2 * p.PO, p.LN), f32),
            pltpu.VMEM((max(p.PO * p.N1, up(p.NM, 128)), p.LN), f32),
            pltpu.VMEM((up(p.NM, 128) // 128, p.B, 128), f32),
            pltpu.VMEM(block, f32),
            pltpu.VMEM(block, f32),
            pltpu.VMEM(block, jnp.int32),
            pltpu.VMEM(block, jnp.int32),
            pltpu.VMEM(block, jnp.int32),
            pltpu.VMEM((p.N2, 2 * p.KO, 2 * p.KA), jnp.bfloat16),
            dma((5,)),
            dma(()),
            dma((3,)),
            dma((3,)),
            dma((2,)),
            dma((2,)),
            dma((1, p.L - 1)),
            dma((1, p.L - 1)),
            dma((p.C, p.L - 1)),
            dma((p.C, p.L - 1)),
        ],
        compiler_params=pltpu.CompilerParams(
            collective_id=0, has_side_effects=True, vmem_limit_bytes=62 * 1024 * 1024
        ),
    )(*args, jnp.asarray(first), jnp.asarray(second))


def solution(mesh):
    field = P(None, "lat", "lon")
    flat = P("lat", "lon")

    def run(*args):
        levels, rows, cols = args[0].shape
        plan = Plan(mesh.shape["lon"], mesh.shape["lat"], levels, rows, cols)
        return body(plan, *args)

    return jax.shard_map(
        run, mesh=mesh, in_specs=(field,) * 5 + (flat,) * 3,
        out_specs=P(None, ("lat", "lon"), None), check_vma=False,
    )
```

```python
import functools

import jax
import jax.numpy as jnp
import numpy as np
from jax import lax
from jax.experimental import pallas as pl
from jax.experimental.pallas import tpu as pltpu
from jax.sharding import PartitionSpec as P

MESH = pl.DeviceIdType.MESH


def up(value, step):
    return -(-value // step) * step


def split_pair(table):
    high = table.astype(jnp.bfloat16)
    low = (table - high.astype(np.float64)).astype(jnp.bfloat16)
    return high, low


class Plan:
    def __init__(self, lon_count, lat_count, levels, rows, cols):
        self.L, self.T, self.K, self.J, self.W = lon_count, lat_count, levels, rows, cols
        self.NI = cols * lon_count
        self.R = rows // lon_count
        best = None
        for n2 in range(2, cols + 1, 2):
            n1 = self.NI // n2
            if cols % n2 or n1 % 4:
                continue
            cost = abs(n1 - 60)
            if best is None or cost < best[0]:
                best = (cost, n2)
        self.N2 = best[1]
        self.N1 = self.NI // self.N2
        self.A = cols // self.N2
        self.AP = up(self.A, 8)
        self.KA = lon_count * self.AP
        self.KO = up(self.N1, 8)
        self.NP = up(self.N2, 8)
        self.PH = self.N2 // 2
        self.parts = [self.N2]
        if self.N2 % 8 == 0 and cols % 8 == 0 and self.N2 >= 48:
            self.parts = [self.N2 - 24, 16, 8]
        self.C = len(self.parts)
        self.starts = [sum(self.parts[:c]) for c in range(self.C)]
        self.U = 4 if self.N2 % 4 == 0 else 2
        self.PO = up(self.PH, 8)
        self.NM = self.NI // 2
        self.WL = up(cols, 128)
        self.WP = up(cols, 8)
        self.B = self.R * levels
        self.LN = up(2 * self.B, 128)
        self.PR = self.AP * self.N2

    def tables(self):
        n = np.arange(self.N2)[:, None, None]
        k = np.arange(self.N1)[None, :, None]
        a = np.arange(self.N1)[None, None, :]
        angle = 2 * np.pi / self.NI * ((k * (self.N2 * a + n)) % self.NI)
        real = np.zeros((self.N2, self.KO, self.L, self.AP))
        imag = np.zeros_like(real)
        real[:, : self.N1, :, : self.A] = np.cos(angle).reshape(self.N2, self.N1, self.L, self.A)
        imag[:, : self.N1, :, : self.A] = -np.sin(angle).reshape(self.N2, self.N1, self.L, self.A)
        first = np.concatenate([real, imag], axis=1).reshape(self.N2, 2 * self.KO, self.KA)
        high, low = split_pair(first)
        first = np.concatenate([high, low], axis=2)
        p = np.arange(self.PH)[:, None]
        m = np.arange(self.N2)[None, :]
        angle = 2 * np.pi / self.N2 * ((p * m) % self.N2)
        second = np.zeros((2, self.PO, 2, self.NP))
        second[0, : self.PH, 0, : self.N2] = np.cos(angle)
        second[0, : self.PH, 1, : self.N2] = np.sin(angle)
        second[1, : self.PH, 0, : self.N2] = -np.sin(angle)
        second[1, : self.PH, 1, : self.N2] = np.cos(angle)
        pieces = []
        for start, size in self.spans():
            piece = second[:, :, :, start : start + size].reshape(2 * self.PO, 2 * size)
            high, low = split_pair(piece)
            piece = np.concatenate([high, low, high], axis=1)
            pieces.append(np.pad(piece, ((0, 0), (0, up(6 * size, 128) - 6 * size))))
        return first, np.concatenate(pieces, axis=1)

    def spans(self):
        every = [(0, self.NP)]
        if self.C > 1:
            every += list(zip(self.starts, self.parts))
        return every

    def span(self, index):
        start, size = self.spans()[index]
        before = sum(up(6 * width, 128) for _, width in self.spans()[:index])
        return start, size, before


def halves(value):
    high = value.astype(jnp.bfloat16)
    low = (value - high.astype(jnp.float32)).astype(jnp.bfloat16)
    return high, low


def kernel(
    p, u_hbm, v_hbm, um_hbm, vm_hbm, tm_hbm, bot_ref, idx_ref, idy_ref, t1_hbm, t2_ref, out_ref,
    mj, adv, inv, south, north, fold, col_out, col_in, send_a, send_b, got_a, got_b, y_ref,
    f_ref, p_ref, g_ref, turned_out, u_ref, v_ref, um_ref, vm_ref, tm_ref, t1, in_sem, table_sem, halo_send, halo_recv, col_send, col_recv, a_send, a_recv,
    b_send, b_recv,
):
    L, K, J, W, WL = p.L, p.K, p.J, p.W, p.WL
    me = lax.axis_index("lon")
    row = lax.axis_index("lat")
    up_lat, down_lat = lax.rem(row + 1, p.T), lax.rem(row + p.T - 1, p.T)
    right, left = lax.rem(me + 1, L), lax.rem(me + L - 1, L)
    partner = L - 1 - me
    at_north = row == p.T - 1

    loads = [
        pltpu.make_async_copy(src, dst, in_sem.at[at])
        for at, (src, dst) in enumerate(
            [(u_hbm, u_ref), (um_hbm, um_ref), (v_hbm, v_ref), (vm_hbm, vm_ref), (tm_hbm, tm_ref)]
        )
    ]
    for load in loads:
        load.start()
    table_copy = pltpu.make_async_copy(t1_hbm, t1, table_sem)
    table_copy.start()

    barrier = pltpu.get_barrier_semaphore()
    for off in range(1, L):
        pl.semaphore_signal(
            barrier, inc=1, device_id={"lon": lax.rem(me + off, L)}, device_id_type=MESH
        )
    for other in (up_lat, down_lat):
        pl.semaphore_signal(barrier, inc=1, device_id={"lat": other}, device_id_type=MESH)

    if WL > W:
        tail = jnp.zeros((2, J, K, WL - W), jnp.float32)
        mj[:, :, :, W:] = tail
        adv[:, :, :, W:] = tail
        inv[:, :, W:] = jnp.zeros((2, J, WL - W), jnp.float32)
    inv[0, :, :W] = idx_ref[...] * 0.5
    inv[1, :, :W] = idy_ref[...] * 0.5
    col_out[...] = jnp.zeros_like(col_out)
    if p.PR > p.WP:
        pad = jnp.zeros((L, p.PR - p.WP, p.LN), jnp.float32)
        got_a[:, p.WP :, :] = pad
        got_b[:, p.WP :, :] = pad
    if p.NP > p.N2:
        y_ref[p.N2 * 2 * p.KO :, :] = jnp.zeros(
            ((p.NP - p.N2) * 2 * p.KO, p.LN), jnp.float32
        )
    for load in loads[:2]:
        load.wait()
    for j in range(J):
        mj[0, j, :, :W] = u_ref[:, j, :] * um_ref[:, j, :].astype(jnp.float32)
    for load in loads[2:4]:
        load.wait()
    for j in range(J):
        mj[1, j, :, :W] = v_ref[:, j, :] * vm_ref[:, j, :].astype(jnp.float32)
    pl.semaphore_wait(barrier, L + 1)

    def remote(src, dst, send, recv, device):
        return pltpu.make_async_remote_copy(
            src_ref=src, dst_ref=dst, send_sem=send, recv_sem=recv, device_id=device,
            device_id_type=MESH,
        )

    to_north = remote(mj.at[:, J - 1], south, halo_send.at[0], halo_recv.at[0], {"lat": up_lat})
    to_south = remote(mj.at[:, 0], north, halo_send.at[1], halo_recv.at[1], {"lat": down_lat})
    to_fold = remote(mj.at[:, J - 1], fold, halo_send.at[2], halo_recv.at[2], {"lon": partner})
    to_right = remote(col_out.at[0], col_in.at[0], col_send.at[0], col_recv.at[0], {"lon": right})
    to_left = remote(col_out.at[1], col_in.at[1], col_send.at[1], col_recv.at[1], {"lon": left})
    def turn(source, target, dest):
        for start in range(0, W, 128):
            pieces = [
                source[f, dest * p.R + r, :, start : start + 128]
                for f in range(2)
                for r in range(p.R)
            ]
            if p.LN > 2 * p.B:
                pieces.append(jnp.zeros((p.LN - 2 * p.B, 128), jnp.float32))
            turned = jnp.transpose(jnp.concatenate(pieces, axis=0))
            size = min(128, p.WP - start)
            target[start : start + size, :] = turned[:size]

    order = sorted(range(1, L), key=lambda off: abs(off - L // 2))

    def exchange(source, buffer, got, send, recv, chunks, after_first=None):
        copies = [[] for _ in range(chunks)]
        for slot, off in enumerate(order):
            dest = lax.rem(me + off, L)
            turn(source, buffer.at[slot], dest)
            for c in range(chunks):
                if chunks == 1:
                    src, dst = buffer.at[slot], got.at[me, pl.ds(0, p.WP)]
                else:
                    part = pl.ds(p.starts[c], p.parts[c])
                    src = buffer.at[slot].reshape(p.A, p.N2, p.LN).at[:, part]
                    dst = got.at[me].reshape(p.AP, p.N2, p.LN).at[pl.ds(0, p.A), part]
                copies[c].append(
                    remote(src, dst, send.at[c, slot], recv.at[c, slot], {"lon": dest})
                )
                if c == 0:
                    copies[c][-1].start()
            if slot == 0 and after_first is not None:
                after_first()
        for group in copies[1:]:
            for copy in group:
                copy.start()
        turn(source, got.at[me], me)
        return copies

    def send_edges():
        for j in range(J):
            for f in range(2):
                col_out[0, f * K : (f + 1) * K, j : j + 1] = mj[f, j, :, W - 1 : W]
                col_out[1, f * K : (f + 1) * K, j : j + 1] = mj[f, j, :, 0:1]
        to_north.start()
        to_south.start()
        to_right.start()
        to_left.start()

        @pl.when(at_north)
        def _():
            to_fold.start()

    copies_a = exchange(mj, send_a, got_a, a_send, a_recv, 1, send_edges)

    to_north.wait()
    to_south.wait()
    to_right.wait()
    to_left.wait()

    @pl.when(at_north)
    def _():
        to_fold.wait()
        line = lax.broadcasted_iota(jnp.int32, (128, 128), 0)
        lane = lax.broadcasted_iota(jnp.int32, (128, 128), 1)
        flip = (line + lane == 127).astype(jnp.float32)
        value = fold[...].reshape(2 * K, WL)
        blocks = [
            jnp.dot(
                value[:, start : start + 128], flip, precision=lax.Precision.HIGHEST,
                preferred_element_type=jnp.float32,
            )
            for start in range(WL - 128, -1, -128)
        ]
        turned = jnp.concatenate(blocks, axis=1)
        if WL > W:
            turned = pltpu.roll(turned, W, 1)
        north[...] = -turned.reshape(2, K, WL)

    @pl.when(row == 0)
    def _():
        south[...] = jnp.zeros_like(south)

    loads[4].wait()
    lane = lax.broadcasted_iota(jnp.int32, (K, WL), 1)
    level = lax.broadcasted_iota(jnp.int32, (K, W), 0)
    for j in range(J):
        here = [mj[f, j] for f in range(2)]
        inv_x = inv[0, j : j + 1, :]
        inv_y = inv[1, j : j + 1, :]
        live = level < bot_ref[j : j + 1, :]
        weight = jnp.where(live, tm_ref[:, j, :].astype(jnp.float32), 0.0)
        for f in range(2):
            below = south[f] if j == 0 else mj[f, j - 1]
            above = north[f] if j == J - 1 else mj[f, j + 1]
            west = jnp.where(
                lane == 0, col_in[0, f * K : (f + 1) * K, j : j + 1], pltpu.roll(here[f], 1, 1)
            )
            east = jnp.where(
                lane == W - 1, col_in[1, f * K : (f + 1) * K, j : j + 1],
                pltpu.roll(here[f], WL - 1, 1),
            )
            slope_x = (east - west) * inv_x
            slope_y = (above - below) * inv_y
            total = here[0] * slope_x + here[1] * slope_y
            adv[f, j, :, :W] = weight * total[:, :W]

    copies_b = exchange(adv, send_b, got_b, b_send, b_recv, p.C)

    table_copy.wait()

    def first_stage(got, begin, end):

        def step(block, carry):
            for part in range(p.U):
                n = block * p.U + part
                x = jnp.concatenate(
                    [got[s, pl.ds(n, p.AP, stride=p.N2), :] for s in range(L)], axis=0
                )
                high, low = halves(x)
                data = jnp.concatenate([high, high, low, low], axis=0)
                table = t1[n]
                out = jnp.dot(
                    jnp.concatenate([table, table], axis=1), data,
                    preferred_element_type=jnp.float32,
                )
                y_ref[pl.ds(pl.multiple_of(n * 2 * p.KO, 8), 2 * p.KO), :] = out
            return carry

        lax.fori_loop(begin // p.U, end // p.U, step, 0)

    def second_stage(finish, index):
        begin, size, before = p.span(index)
        table = t2_ref[:, before : before + 6 * size]

        def step(block, carry):
            for part in range(2):
                ks = [block * 4 + part * 2 + q for q in range(2)]
                sides = []
                for k in ks:
                    y = jnp.concatenate(
                        [
                            y_ref[pl.ds(2 * p.KO * begin + k + c * p.KO, size, stride=2 * p.KO), :]
                            for c in range(2)
                        ],
                        axis=0,
                    )
                    high, low = halves(y)
                    sides.append(jnp.concatenate([high, high, low], axis=0))
                out = jnp.dot(
                    table, jnp.concatenate(sides, axis=1), preferred_element_type=jnp.float32
                )
                for q, k in enumerate(ks):
                    finish(k, out[:, q * p.LN : (q + 1) * p.LN])
            return carry

        lax.fori_loop(0, p.N1 // 4, step, 0)

    def keep(k, value):
        f_ref[k] = value

    def begin_sum(k, value):
        p_ref[k] = value

    def add_sum(k, value):
        p_ref[k] += value

    def cross(k, value):
        both = f_ref[k] * (value if p.C == 1 else p_ref[k] + value)
        g_ref[pl.ds(k, p.PO, stride=p.N1), :] = both[: p.PO] + both[p.PO :]

    for copy in copies_a[0]:
        copy.wait()
    first_stage(got_a, 0, p.N2)
    second_stage(keep, 0)
    for c, group in enumerate(copies_b):
        for copy in group:
            copy.wait()
        first_stage(got_b, p.starts[c], p.starts[c] + p.parts[c])
        finish = cross if c == p.C - 1 else begin_sum if c == 0 else add_sum
        second_stage(finish, c + 1 if p.C > 1 else 0)

    for start in range(0, p.NM, 128):
        size = min(128, p.NM - start)
        block = jnp.transpose(g_ref[start : start + 128, :])
        wave = lax.broadcasted_iota(jnp.int32, (p.B, 128), 1) + start
        scale = jnp.where(wave == 0, -1.0 / p.NI, -2.0 / p.NI)
        total = (block[: p.B] + block[p.B : 2 * p.B]) * scale
        turned_out[start // 128] = total
        for k in range(p.K):
            rows = turned_out[start // 128, pl.ds(k, p.R, stride=p.K), :]
            out_ref[k, :, start : start + size] = rows[:, :size]


def body(p, *args):
    first, second = p.tables()
    f32 = jnp.float32
    vmem = pl.BlockSpec(memory_space=pltpu.VMEM)
    hbm = pl.BlockSpec(memory_space=pl.ANY)
    dma = pltpu.SemaphoreType.DMA
    block = (p.K, p.J, p.W)
    return pl.pallas_call(
        functools.partial(kernel, p),
        out_shape=jax.ShapeDtypeStruct((p.K, p.R, p.NM), f32),
        in_specs=[hbm] * 5 + [vmem] * 3 + [hbm, vmem],
        out_specs=vmem,
        scratch_shapes=[
            pltpu.VMEM((2, p.J, p.K, p.WL), f32),
            pltpu.VMEM((2, p.J, p.K, p.WL), f32),
            pltpu.VMEM((2, p.J, p.WL), f32),
            pltpu.VMEM((2, p.K, p.WL), f32),
            pltpu.VMEM((2, p.K, p.WL), f32),
            pltpu.VMEM((2, p.K, p.WL), f32),
            pltpu.VMEM((2, 2 * p.K, 128), f32),
            pltpu.VMEM((2, 2 * p.K, 128), f32),
            pltpu.VMEM((p.L - 1, p.WP, p.LN), f32),
            pltpu.VMEM((p.L - 1, p.WP, p.LN), f32),
            pltpu.VMEM((p.L, p.PR, p.LN), f32),
            pltpu.VMEM((p.L, p.PR, p.LN), f32),
            pltpu.VMEM((p.NP * 2 * p.KO, p.LN), f32),
            pltpu.VMEM((p.N1, 2 * p.PO, p.LN), f32),
            pltpu.VMEM((p.N1, 2 * p.PO, p.LN), f32),
            pltpu.VMEM((max(p.PO * p.N1, up(p.NM, 128)), p.LN), f32),
            pltpu.VMEM((up(p.NM, 128) // 128, p.B, 128), f32),
            pltpu.VMEM(block, f32),
            pltpu.VMEM(block, f32),
            pltpu.VMEM(block, jnp.int32),
            pltpu.VMEM(block, jnp.int32),
            pltpu.VMEM(block, jnp.int32),
            pltpu.VMEM((p.N2, 2 * p.KO, 2 * p.KA), jnp.bfloat16),
            dma((5,)),
            dma(()),
            dma((3,)),
            dma((3,)),
            dma((2,)),
            dma((2,)),
            dma((1, p.L - 1)),
            dma((1, p.L - 1)),
            dma((p.C, p.L - 1)),
            dma((p.C, p.L - 1)),
        ],
        compiler_params=pltpu.CompilerParams(
            collective_id=0, has_side_effects=True, vmem_limit_bytes=62 * 1024 * 1024
        ),
    )(*args, jnp.asarray(first), jnp.asarray(second))


def solution(mesh):
    field = P(None, "lat", "lon")
    flat = P("lat", "lon")

    def run(*args):
        levels, rows, cols = args[0].shape
        plan = Plan(mesh.shape["lon"], mesh.shape["lat"], levels, rows, cols)
        return body(plan, *args)

    return jax.shard_map(
        run, mesh=mesh, in_specs=(field,) * 5 + (flat,) * 3,
        out_specs=P(None, ("lat", "lon"), None), check_vma=False,
    )
```
